8 devices in a mesh: dp: 1 (over z), sp: 8 (over y, x, core).
Axes of the slice: x: 2, y: 2, z: 1, core: 2. Of those that a mesh axis runs over, the one named last changes fastest.
Arguments:
- dec_hidden: bfloat16 [2048, 4096], P(('dp', 'sp'))
- enc_memory: bfloat16 [8192, 4096], P(('dp', 'sp'))
- mem_len: int32 [1], P('dp')
- norm_self: bfloat16 [2, 4096], replicated
- norm_cross: bfloat16 [2, 4096], replicated
- norm_mlp: bfloat16 [2, 4096], replicated
- self_q: bfloat16 [2, 4096, 4096], replicated
- self_k: bfloat16 [2, 4096, 4096], replicated
- self_v: bfloat16 [2, 4096, 4096], replicated
- self_o: bfloat16 [2, 32, 128, 4096], replicated
- cross_q: bfloat16 [2, 4096, 4096], replicated
- cross_k: bfloat16 [2, 4096, 1024], replicated
- cross_v: bfloat16 [2, 4096, 1024], replicated
- cross_o: bfloat16 [2, 32, 128, 4096], replicated
- mlp_gate: bfloat16 [2, 4096, 14336], replicated
- mlp_up: bfloat16 [2, 4096, 14336], replicated
- mlp_down: bfloat16 [2, 14336, 4096], replicated
Outputs:
- output: bfloat16 [2048, 4096], P(('dp', 'sp'))
All inputs are finite; a program needn't handle non-finite values.
Results may differ from the reference program's by a relative error of at most 0.0127063.
Values are sent between devices in bfloat16 or wider.
A program may use at most 4.5 GiB of HBM per device.

```python
import jax
import jax.numpy as jnp
from jax import lax

D = 4096
HEADS = 32
KV_HEADS = 8
HEAD = 128
FF = 14336
LAYERS = 2
TQ = 2048
TM = 8192
WAVES = 4
EPS = 1e-6
NEG_BIG = -1e30
SOFT_SCALE = HEAD ** -0.5
DKV = KV_HEADS * HEAD


def smooth_field(wave_key, n_rows, n_cols):
    directions = jax.random.normal(wave_key, (WAVES, n_cols), jnp.float32)
    positions = jnp.arange(n_rows, dtype=jnp.float32) / n_rows
    freq_list = jnp.arange(1, WAVES + 1, dtype=jnp.float32)
    wave_rows = jnp.cos(jnp.pi * positions[:, None] * freq_list[None, :])
    return jnp.dot(wave_rows, directions)


def setup_inputs(seed: int = 0, part: int = 0) -> dict:
    part_key = jax.random.fold_in(jax.random.key(seed), part)
    part_keys = jax.random.split(part_key, 5)
    shared = jax.random.split(jax.random.key(seed + 1), 16)

    def weight(key_index, shape_tail, fan_in):
        raw_draw = jax.random.normal(shared[key_index], (LAYERS,) + shape_tail, jnp.float32)
        return (raw_draw * fan_in ** -0.5).astype(jnp.bfloat16)

    def gain(key_index):
        return jax.random.uniform(shared[key_index], (LAYERS, D), jnp.float32, 0.5, 1.5).astype(jnp.bfloat16)

    dec_hidden = jax.random.normal(part_keys[0], (TQ, D), jnp.float32) + smooth_field(part_keys[1], TQ, D)
    enc_memory = jax.random.normal(part_keys[2], (TM, D), jnp.float32) + smooth_field(part_keys[3], TM, D)
    mem_len = jax.random.randint(part_keys[4], (1,), TM // 4, 3 * TM // 4 + 1, dtype=jnp.int32)
    return {
        'dec_hidden': dec_hidden.astype(jnp.bfloat16),
        'enc_memory': enc_memory.astype(jnp.bfloat16),
        'mem_len': mem_len,
        'norm_self': gain(0),
        'norm_cross': gain(1),
        'norm_mlp': gain(2),
        'self_q': weight(3, (D, D), D),
        'self_k': weight(4, (D, D), D),
        'self_v': weight(5, (D, D), D),
        'self_o': weight(6, (HEADS, HEAD, D), D),
        'cross_q': weight(7, (D, D), D),
        'cross_k': weight(8, (D, DKV), D),
        'cross_v': weight(9, (D, DKV), D),
        'cross_o': weight(10, (HEADS, HEAD, D), D),
        'mlp_gate': weight(11, (D, FF), D),
        'mlp_up': weight(12, (D, FF), D),
        'mlp_down': weight(13, (FF, D), FF),
    }


def rms_norm(hidden, gain_vec):
    hidden32 = hidden.astype(jnp.float32)
    inv_rms = lax.rsqrt(jnp.mean(hidden32 * hidden32, axis=-1, keepdims=True) + EPS)
    return (hidden32 * inv_rms * gain_vec.astype(jnp.float32)).astype(jnp.bfloat16)


def project(acts, weight_mat):
    return jnp.dot(acts, weight_mat, preferred_element_type=jnp.float32).astype(jnp.bfloat16)


def add_residual(hidden, update):
    return (hidden.astype(jnp.float32) + update).astype(jnp.bfloat16)


def head_attend(query_h, key_h, value_h, allowed):
    scores = jnp.dot(query_h, key_h.T, preferred_element_type=jnp.float32) * SOFT_SCALE
    scores = jnp.where(allowed, scores, NEG_BIG)
    weights = jnp.exp(scores - jnp.max(scores, axis=-1, keepdims=True))
    numerator = jnp.dot(weights.astype(jnp.bfloat16), value_h, preferred_element_type=jnp.float32)
    return numerator / jnp.sum(weights, axis=-1, keepdims=True)


def multi_head(queries, keys_all, values_all, allowed):
    q_rows = queries.shape[0]
    k_rows = keys_all.shape[0]
    kv_count = keys_all.shape[1] // HEAD
    q_heads = queries.reshape(q_rows, HEADS, HEAD).transpose(1, 0, 2)
    k_heads = jnp.repeat(keys_all.reshape(k_rows, kv_count, HEAD).transpose(1, 0, 2), HEADS // kv_count, axis=0)
    v_heads = jnp.repeat(values_all.reshape(k_rows, kv_count, HEAD).transpose(1, 0, 2), HEADS // kv_count, axis=0)
    per_head = lax.map(lambda head_trio: head_attend(head_trio[0], head_trio[1], head_trio[2], allowed), (q_heads, k_heads, v_heads))
    return per_head.transpose(1, 0, 2).astype(jnp.bfloat16)


def reference(dec_hidden, enc_memory, mem_len, norm_self, norm_cross, norm_mlp, self_q, self_k, self_v, self_o, cross_q, cross_k, cross_v, cross_o, mlp_gate, mlp_up, mlp_down):
    causal = jnp.arange(TQ)[:, None] >= jnp.arange(TQ)[None, :]
    mem_valid = (jnp.arange(TM) < mem_len[0])[None, :]
    stacked = {
        'norm_self': norm_self, 'norm_cross': norm_cross, 'norm_mlp': norm_mlp,
        'self_q': self_q, 'self_k': self_k, 'self_v': self_v, 'self_o': self_o,
        'cross_q': cross_q, 'cross_k': cross_k, 'cross_v': cross_v, 'cross_o': cross_o,
        'mlp_gate': mlp_gate, 'mlp_up': mlp_up, 'mlp_down': mlp_down,
    }

    def layer_step(hidden, params):
        normed = rms_norm(hidden, params['norm_self'])
        attended = multi_head(project(normed, params['self_q']), project(normed, params['self_k']), project(normed, params['self_v']), causal)
        update = jnp.einsum('thd,hdo->to', attended.astype(jnp.float32), params['self_o'].astype(jnp.float32))
        hidden = add_residual(hidden, update)
        normed = rms_norm(hidden, params['norm_cross'])
        attended = multi_head(project(normed, params['cross_q']), project(enc_memory, params['cross_k']), project(enc_memory, params['cross_v']), mem_valid)
        update = jnp.einsum('thd,hdo->to', attended.astype(jnp.float32), params['cross_o'].astype(jnp.float32))
        hidden = add_residual(hidden, update)
        normed = rms_norm(hidden, params['norm_mlp'])
        gate_pre = jnp.dot(normed, params['mlp_gate'], preferred_element_type=jnp.float32)
        up_proj = jnp.dot(normed, params['mlp_up'], preferred_element_type=jnp.float32)
        hidden_act = (jax.nn.silu(gate_pre) * up_proj).astype(jnp.bfloat16)
        update = jnp.dot(hidden_act, params['mlp_down'], preferred_element_type=jnp.float32)
        return add_residual(hidden, update), None

    final_hidden, _ = lax.scan(layer_step, dec_hidden, stacked)
    return final_hidden
```

```python
import functools

import jax
import jax.numpy as jnp
from jax import lax
from jax.experimental import pallas as pl
from jax.experimental.pallas import tpu as pltpu
from jax.sharding import PartitionSpec as P

EPS = 1e-6
NEG_BIG = -1e30
LOG2E = 1.4426950408889634
MESH = pl.DeviceIdType.MESH
VMEM_LIMIT = 66_000_000
BF16 = jnp.bfloat16
F32 = jnp.float32


def norm_rows(hidden, gain):
    h = hidden.astype(F32)
    inv = lax.rsqrt(jnp.mean(h * h, axis=-1, keepdims=True) + EPS)
    return (h * inv * gain.astype(F32)).astype(BF16)


def dot(a, b):
    return jnp.dot(a, b, preferred_element_type=F32)


def dot_t(a, b):
    return lax.dot_general(a, b, (((1,), (1,)), ((), ())), preferred_element_type=F32)


def params(collective_id, dims=1):
    return pltpu.CompilerParams(
        collective_id=collective_id,
        has_side_effects=collective_id is not None,
        vmem_limit_bytes=VMEM_LIMIT,
        dimension_semantics=("arbitrary",) * dims,
    )


class Exchange:
    def __init__(self, group):
        self.group = group
        self.me = lax.axis_index("sp")
        self.dp = lax.axis_index("dp")

    def peer(self, offset):
        return lax.rem(self.me + offset, self.group)

    def greet(self):
        barrier = pltpu.get_barrier_semaphore()
        for k in range(1, self.group):
            pl.semaphore_signal(
                barrier, inc=1, device_id=(self.dp, self.peer(k)), device_id_type=MESH
            )

    def await_all(self):
        pl.semaphore_wait(pltpu.get_barrier_semaphore(), self.group - 1)

    def copy(self, src, dst, send, recv, target):
        return pltpu.make_async_remote_copy(
            src_ref=src, dst_ref=dst, send_sem=send, recv_sem=recv,
            device_id=(self.dp, target), device_id_type=MESH,
        )


def qkv_kernel(group, layer, mem_layers, refs):
    n_w = 3
    it = iter(refs)
    hid, gain = next(it), next(it)
    w = [next(it) for _ in range(n_w)]
    if mem_layers:
        mem, ck, cv = next(it), next(it), next(it)
    out = next(it)
    if mem_layers:
        kv_out, kv_keep = next(it), next(it)
    x, buf, ssem, rsem, lsem = (next(it) for _ in range(5))
    if mem_layers:
        mem_v, kv_buf, kv_buf1, kvs, kvr, kvl, keep_sem, mem_sem = (next(it) for _ in range(8))
    ex = Exchange(group)
    me = ex.me
    i = pl.program_id(0)
    rows = hid.shape[0]
    width = buf.shape[2]
    half = width // 2
    n_steps = n_w * group * 2

    @pl.when(i == 0)
    def _():
        ex.greet()
        if mem_layers:
            pltpu.make_async_copy(mem, mem_v, mem_sem).start()
        x[...] = norm_rows(hid[...], gain[layer : layer + 1, :])

    @pl.when(i == 1)
    def _():
        ex.await_all()

    for t in range(n_w):

        @pl.when((i >= t * group * 2) & (i < (t + 1) * group * 2))
        def _(t=t):
            slot = lax.div(i, 2)
            res = dot(x[...], w[t][0]).astype(BF16)

            @pl.when(lax.rem(i, 2) == 0)
            def _():
                buf[slot, :, 0:half] = res

            @pl.when(lax.rem(i, 2) == 1)
            def _():
                buf[slot, :, half:width] = res

    def out_at(t, p):
        return out.at[t, pl.ds(pl.multiple_of(p * rows, rows), rows)]

    def block_copy(slot):
        t, r = lax.div(slot, group), lax.rem(slot, group)
        return t, r, ex.copy(
            buf.at[slot], out_at(t, me), ssem.at[slot], rsem.at[t, me], ex.peer(r + 1)
        )

    def own_copy(t):
        return pltpu.make_async_copy(buf.at[t * group + group - 1], out_at(t, me), lsem.at[t])

    @pl.when((i >= 2) & (i <= n_steps) & (lax.rem(i, 2) == 0))
    def _():
        slot = lax.div(i, 2) - 1
        t, r, cp = block_copy(slot)

        @pl.when(r < group - 1)
        def _():
            cp.start()

        @pl.when(r == group - 1)
        def _():
            own_copy(t).start()

    last = n_steps
    if mem_layers:
        pairs = group // 2
        hd = ck.shape[2] // 2
        mem_rows = mem.shape[0]
        senders = kv_out.shape[0]
        base = n_steps
        last = n_steps + mem_layers * pairs * 2

        @pl.when(i == base)
        def _():
            pltpu.make_async_copy(mem, mem_v, mem_sem).wait()

        bufs = (kv_buf, kv_buf1)
        for m in range(mem_layers):
            b0 = base + m * pairs * 2

            @pl.when((i >= b0) & (i < b0 + pairs * 2))
            def _(m=m, b0=b0):
                j = i - b0
                pair = lax.div(j, 2)
                for kind, wref in enumerate((ck, cv)):

                    @pl.when((lax.rem(j, 2) == kind) & (me < senders))
                    def _(kind=kind, wref=wref):
                        for c in range(4):
                            q4 = mem_rows // 4
                            rs = slice(c * q4, (c + 1) * q4)
                            res = dot(mem_v[rs, :], wref[0]).astype(BF16)
                            for side in range(2):
                                bufs[m][2 * pair + side, rs, kind * hd : (kind + 1) * hd] = res[
                                    :, side * hd : (side + 1) * hd
                                ]

        def kv_copy(d):
            return ex.copy(kv_buf.at[d], kv_out.at[me], kvs.at[d], kvr.at[me], d)

        @pl.when((i > base) & (i <= base + pairs * 2) & (lax.rem(i - base, 2) == 0) & (me < senders))
        def _():
            pair = lax.div(i - base, 2) - 1
            for side in range(2):
                d = 2 * pair + side

                @pl.when(d != me)
                def _():
                    kv_copy(d).start()

                @pl.when(d == me)
                def _():
                    pltpu.make_async_copy(kv_buf.at[d], kv_out.at[me], kvl).start()

        keep_copy = pltpu.make_async_copy(kv_buf1, kv_keep, keep_sem)

        @pl.when(i == last)
        def _():
            keep_copy.start()

    @pl.when(i == last)
    def _():
        for t in range(n_w):
            own_copy(t).wait()
            for k in range(1, group):
                p = ex.peer(k)
                ex.copy(buf.at[0], out_at(t, p), ssem.at[t * group + k - 1], rsem.at[t, p], p).wait()
        if mem_layers:

            @pl.when(me < senders)
            def _():
                pltpu.make_async_copy(kv_buf.at[0], kv_out.at[me], kvl).wait()
                for k in range(1, group):
                    kv_copy(ex.peer(k)).wait_send()

            for p in range(senders):

                @pl.when(me != p)
                def _(p=p):
                    ex.copy(kv_buf.at[0], kv_out.at[p], kvs.at[0], kvr.at[p], p).wait_recv()

            keep_copy.wait()


def qkv_call(mesh, layer, hidden, gain, ws, mem=None, ck=None, cv=None):
    group = mesh.shape["sp"]
    rows, width = hidden.shape
    per_dev = ws[0].shape[2] // group
    tn = per_dev // 2
    n_steps = 3 * group * 2
    mem_layers = 0 if mem is None else ck.shape[0]

    def w_map(t):
        def index(i):
            j = jnp.clip(i - t * group * 2, 0, group * 2 - 1)
            d = lax.rem(lax.axis_index("sp") + 1 + lax.div(j, 2), group)
            return layer, 0, d * 2 + lax.rem(j, 2)

        return index

    in_specs = [
        pl.BlockSpec((rows, width), lambda i: (0, 0), pipeline_mode=pl.Buffered(1)),
        pl.BlockSpec(gain.shape, lambda i: (0, 0), pipeline_mode=pl.Buffered(1)),
    ] + [pl.BlockSpec((1, width, tn), w_map(t)) for t in range(3)]
    args = [hidden, gain, *ws]
    out_shape = [jax.ShapeDtypeStruct((3, rows * group, per_dev), BF16)]
    scratch = [
        pltpu.VMEM((rows, width), BF16),
        pltpu.VMEM((3 * group, rows, per_dev), BF16),
        pltpu.SemaphoreType.DMA((3 * group,)),
        pltpu.SemaphoreType.DMA((3, group)),
        pltpu.SemaphoreType.DMA((3,)),
    ]
    last = n_steps
    if mem_layers:
        mem_rows = mem.shape[0]
        hd = ck.shape[2] // group
        pairs = group // 2
        senders = group * 3 // 4

        def kv_map(i):
            j = jnp.clip(i - n_steps, 0, mem_layers * pairs * 2 - 1)
            return lax.div(j, pairs * 2), 0, lax.div(lax.rem(j, pairs * 2), 2)

        in_specs += [
            pl.BlockSpec(memory_space=pl.ANY),
            pl.BlockSpec((1, width, 2 * hd), kv_map),
            pl.BlockSpec((1, width, 2 * hd), kv_map),
        ]
        args += [mem, ck, cv]
        out_shape += [
            jax.ShapeDtypeStruct((senders, mem_rows, 2 * hd), BF16),
            jax.ShapeDtypeStruct((group, mem_rows, 2 * hd), BF16),
        ]
        scratch += [
            pltpu.VMEM((mem_rows, width), BF16),
            pltpu.VMEM((group, mem_rows, 2 * hd), BF16),
            pltpu.VMEM((group, mem_rows, 2 * hd), BF16),
            pltpu.SemaphoreType.DMA((group,)),
            pltpu.SemaphoreType.DMA((group,)),
            pltpu.SemaphoreType.DMA,
            pltpu.SemaphoreType.DMA,
            pltpu.SemaphoreType.DMA,
        ]
        last = n_steps + mem_layers * pairs * 2

    def body(*refs):
        qkv_kernel(group, layer, mem_layers, refs)

    return pl.pallas_call(
        body,
        grid=(last + 1,),
        in_specs=in_specs,
        out_specs=[pl.BlockSpec(memory_space=pl.ANY)] * len(out_shape),
        out_shape=out_shape,
        scratch_shapes=scratch,
        compiler_params=params(layer),
        name=f"qkv{layer}",
    )(*args)


def send_back(ex, i, group, rows, cols, buf, out, ssem, rsem, lsem):
    me = ex.me

    def out_at(p):
        return out.at[:, pl.ds(pl.multiple_of(p * cols, cols), cols)]

    own = pltpu.make_async_copy(buf.at[group - 1], out_at(me), lsem)

    @pl.when((i >= 1) & (i < group))
    def _():
        r = i - 1
        ex.copy(buf.at[r], out_at(me), ssem.at[r], rsem.at[me], ex.peer(r + 1)).start()

    @pl.when(i == group)
    def _():
        own.start()
        for k in range(1, group):
            p = ex.peer(k)
            ex.copy(buf.at[k - 1], out_at(p), ssem.at[k - 1], rsem.at[p], p).wait()
        own.wait()


def self_kernel(group, hd, qkv, out, buf, ssem, rsem, lsem, m_s, l_s, acc_s):
    ex = Exchange(group)
    i = pl.program_id(0)
    rows, cols = buf.shape[1], buf.shape[2]
    heads = cols // hd
    bk = 2 * rows
    coef = hd**-0.5 * LOG2E

    @pl.when(i == 0)
    def _():
        ex.greet()

    @pl.when(i == 1)
    def _():
        ex.await_all()

    @pl.when(i < group)
    def _():
        d = ex.peer(i + 1)
        r0 = pl.multiple_of(d * rows, rows)
        for h in range(heads):
            m_s[h] = jnp.full((rows, 1), NEG_BIG, F32)
            l_s[h] = jnp.zeros((rows, 1), F32)
            acc_s[h] = jnp.zeros((rows, hd), F32)

        def step(kb, masked):
            k0 = pl.multiple_of(kb * bk, bk)
            if masked:
                row = r0 + lax.broadcasted_iota(jnp.int32, (rows, bk), 0)
                col = k0 + lax.broadcasted_iota(jnp.int32, (rows, bk), 1)
                allowed = row >= col
            for h in range(heads):
                hs = slice(h * hd, (h + 1) * hd)
                s = dot_t(qkv[0, pl.ds(r0, rows), hs], qkv[1, pl.ds(k0, bk), hs])
                if masked:
                    s = jnp.where(allowed, s, NEG_BIG)
                m_old = m_s[h]
                m_new = jnp.maximum(m_old, jnp.max(s, axis=-1, keepdims=True))
                p = jnp.exp2((s - m_new) * coef)
                alpha = jnp.exp2((m_old - m_new) * coef)
                l_s[h] = l_s[h] * alpha + jnp.sum(p, axis=-1, keepdims=True)
                acc_s[h] = acc_s[h] * alpha + dot(p.astype(BF16), qkv[2, pl.ds(k0, bk), hs])
                m_s[h] = m_new

        full = lax.div(d, 2)

        def loop(kb, c):
            step(kb, False)
            return c

        lax.fori_loop(0, full, loop, 0)
        step(full, True)
        for h in range(heads):
            buf[i, :, h * hd : (h + 1) * hd] = (acc_s[h] / l_s[h]).astype(BF16)

    send_back(ex, i, group, rows, cols, buf, out, ssem, rsem, lsem)


def back_scratch(group, rows, cols):
    return [
        pltpu.VMEM((group, rows, cols), BF16),
        pltpu.SemaphoreType.DMA((group,)),
        pltpu.SemaphoreType.DMA((group,)),
        pltpu.SemaphoreType.DMA,
    ]


def self_call(mesh, hd, qkv, cid):
    group = mesh.shape["sp"]
    _, all_rows, cols = qkv.shape
    rows = all_rows // group
    heads = cols // hd
    return pl.pallas_call(
        functools.partial(self_kernel, group, hd),
        grid=(group + 1,),
        in_specs=[pl.BlockSpec(qkv.shape, lambda i: (0, 0, 0), pipeline_mode=pl.Buffered(1))],
        out_specs=pl.BlockSpec(memory_space=pl.ANY),
        out_shape=jax.ShapeDtypeStruct((rows, cols * group), BF16),
        scratch_shapes=back_scratch(group, rows, cols)
        + [
            pltpu.VMEM((heads, rows, 1), F32),
            pltpu.VMEM((heads, rows, 1), F32),
            pltpu.VMEM((heads, rows, hd), F32),
        ],
        compiler_params=params(cid),
        name="self_attn",
    )(qkv)


def cross_kernel(group, hd, bk, mem_len, q, kv, out, buf, ssem, rsem, lsem, m_s, l_s, acc_s):
    ex = Exchange(group)
    i = pl.program_id(0)
    rows, cols = buf.shape[1], buf.shape[2]
    heads = cols // hd
    coef = hd**-0.5 * LOG2E
    n_kb = kv.shape[0] // bk

    @pl.when(i == 0)
    def _():
        ex.greet()

    @pl.when(i == 1)
    def _():
        ex.await_all()

    @pl.when(i < group)
    def _():
        d = ex.peer(i + 1)
        r0 = pl.multiple_of(d * rows, rows)
        for h in range(heads):
            m_s[h] = jnp.full((rows, 1), NEG_BIG, F32)
            l_s[h] = jnp.zeros((rows, 1), F32)
            acc_s[h] = jnp.zeros((rows, hd), F32)

        def loop(kb, c):
            k0 = pl.multiple_of(kb * bk, bk)
            col = k0 + lax.broadcasted_iota(jnp.int32, (1, bk), 1)
            allowed = col < mem_len[0]
            keys = kv[pl.ds(k0, bk), 0:hd]
            vals = kv[pl.ds(k0, bk), hd : 2 * hd]
            for h in range(heads):
                s = dot_t(q[pl.ds(r0, rows), h * hd : (h + 1) * hd], keys)
                s = jnp.where(allowed, s, NEG_BIG)
                m_old = m_s[h]
                m_new = jnp.maximum(m_old, jnp.max(s, axis=-1, keepdims=True))
                p = jnp.exp2((s - m_new) * coef)
                alpha = jnp.exp2((m_old - m_new) * coef)
                l_s[h] = l_s[h] * alpha + jnp.sum(p, axis=-1, keepdims=True)
                acc_s[h] = acc_s[h] * alpha + dot(p.astype(BF16), vals)
                m_s[h] = m_new
            return c

        lax.fori_loop(0, n_kb, loop, 0)
        for h in range(heads):
            buf[i, :, h * hd : (h + 1) * hd] = (acc_s[h] / l_s[h]).astype(BF16)

    send_back(ex, i, group, rows, cols, buf, out, ssem, rsem, lsem)


def cross_call(mesh, hd, mem_len, q, kv, cid):
    group = mesh.shape["sp"]
    all_rows, cols = q.shape
    rows = all_rows // group
    heads = cols // hd
    return pl.pallas_call(
        functools.partial(cross_kernel, group, hd, 1024),
        grid=(group + 1,),
        in_specs=[
            pl.BlockSpec(memory_space=pltpu.SMEM),
            pl.BlockSpec(q.shape, lambda i: (0, 0), pipeline_mode=pl.Buffered(1)),
            pl.BlockSpec(kv.shape, lambda i: (0, 0), pipeline_mode=pl.Buffered(1)),
        ],
        out_specs=pl.BlockSpec(memory_space=pl.ANY),
        out_shape=jax.ShapeDtypeStruct((rows, cols * group), BF16),
        scratch_shapes=back_scratch(group, rows, cols)
        + [
            pltpu.VMEM((heads, rows, 1), F32),
            pltpu.VMEM((heads, rows, 1), F32),
            pltpu.VMEM((heads, rows, hd), F32),
        ],
        compiler_params=params(cid),
        name="cross_attn",
    )(mem_len, q, kv)


def cross_q_kernel(group, layer, att, hid, gain, wo, wq, out, q_out, x, buf, ssem, rsem, lsem):
    ex = Exchange(group)
    me = ex.me
    i = pl.program_id(0)
    rows = hid.shape[0]
    tn = wo.shape[2]
    n_o = hid.shape[1] // tn

    @pl.when(i == 0)
    def _():
        ex.greet()

    for t in range(n_o):

        @pl.when(i == t)
        def _(t=t):
            cs = slice(t * tn, (t + 1) * tn)
            out[:, cs] = (hid[:, cs].astype(F32) + dot(att[...], wo[0])).astype(BF16)

    @pl.when(i == n_o)
    def _():
        ex.await_all()
        x[...] = norm_rows(out[...], gain[layer : layer + 1, :])

    def out_at(p):
        return q_out.at[pl.ds(pl.multiple_of(p * rows, rows), rows)]

    own = pltpu.make_async_copy(buf.at[group - 1], out_at(me), lsem)

    @pl.when((i >= n_o) & (i < n_o + group))
    def _():
        buf[i - n_o] = dot(x[...], wq[0]).astype(BF16)

    @pl.when((i > n_o) & (i < n_o + group))
    def _():
        r = i - n_o - 1
        ex.copy(buf.at[r], out_at(me), ssem.at[r], rsem.at[me], ex.peer(r + 1)).start()

    @pl.when(i == n_o + group)
    def _():
        own.start()
        for k in range(1, group):
            p = ex.peer(k)
            ex.copy(buf.at[k - 1], out_at(p), ssem.at[k - 1], rsem.at[p], p).wait()
        own.wait()


def cross_q_call(mesh, layer, att, hidden, gain, wo, wq, cid):
    group = mesh.shape["sp"]
    rows, width = hidden.shape
    tn = wq.shape[2] // group
    n_o = width // tn
    whole = pl.BlockSpec((rows, width), lambda i: (0, 0), pipeline_mode=pl.Buffered(1))

    def q_map(i):
        j = jnp.clip(i - n_o, 0, group - 1)
        return layer, 0, lax.rem(lax.axis_index("sp") + 1 + j, group)

    return pl.pallas_call(
        functools.partial(cross_q_kernel, group, layer),
        grid=(n_o + group + 1,),
        in_specs=[
            whole,
            whole,
            pl.BlockSpec(gain.shape, lambda i: (0, 0), pipeline_mode=pl.Buffered(1)),
            pl.BlockSpec((1, width, tn), lambda i: (layer, 0, jnp.minimum(i, n_o - 1))),
            pl.BlockSpec((1, width, tn), q_map),
        ],
        out_specs=[pl.BlockSpec((rows, width), lambda i: (0, 0)), pl.BlockSpec(memory_space=pl.ANY)],
        out_shape=[
            jax.ShapeDtypeStruct((rows, width), BF16),
            jax.ShapeDtypeStruct((rows * group, tn), BF16),
        ],
        scratch_shapes=[pltpu.VMEM((rows, width), BF16)] + back_scratch(group, rows, tn),
        compiler_params=params(cid),
        name=f"cross_q{layer}",
    )(att, hidden, gain, wo, wq)


def post_kernel(group, layer, counts, senders, refs):
    n_o, n_f, n_d = counts
    it = iter(refs)
    att, hid, gain, wo, wg, wu, wd = (next(it) for _ in range(7))
    keep = next(it) if senders else None
    out = next(it)
    kv_out = next(it) if senders else None
    y, x, act = (next(it) for _ in range(3))
    i = pl.program_id(0)
    tn = wo.shape[2]
    td = wd.shape[2]
    last = n_o + n_f + n_d - 1
    if senders:
        kvs, kvr, kvl = (next(it) for _ in range(3))
        ex = Exchange(group)
        me = ex.me

        def kv_copy(d):
            return ex.copy(keep.at[d], kv_out.at[me], kvs.at[d], kvr.at[me], d)

        own = pltpu.make_async_copy(keep.at[me], kv_out.at[me], kvl)

        @pl.when(i == 0)
        def _():
            ex.greet()

        @pl.when(i == 1)
        def _():
            ex.await_all()

        @pl.when((i == 1) & (me < senders))
        def _():
            own.start()
            for k in range(1, group):
                kv_copy(ex.peer(k)).start()

    for t in range(n_o):

        @pl.when(i == t)
        def _(t=t):
            cs = slice(t * tn, (t + 1) * tn)
            y[:, cs] = (hid[:, cs].astype(F32) + dot(att[...], wo[0])).astype(BF16)

    @pl.when(i == n_o)
    def _():
        x[...] = norm_rows(y[...], gain[layer : layer + 1, :])

    @pl.when((i >= n_o) & (i < n_o + n_f))
    def _():
        g = dot(x[...], wg[0])
        u = dot(x[...], wu[0])
        act[i - n_o] = (g * jax.nn.sigmoid(g) * u).astype(BF16)

    tf = wg.shape[2]
    for t in range(n_d):

        @pl.when(i == n_o + n_f + t)
        def _(t=t):
            cs = slice(t * td, (t + 1) * td)
            total = y[:, cs].astype(F32)
            acc = dot(act[0], wd[0, 0:tf, :])
            for c in range(1, n_f):
                acc += dot(act[c], wd[0, c * tf : (c + 1) * tf, :])
            out[:, cs] = (total + acc).astype(BF16)

    if senders:

        @pl.when(i == last)
        def _():
            @pl.when(me < senders)
            def _():
                own.wait()
                for k in range(1, group):
                    kv_copy(ex.peer(k)).wait_send()

            for p in range(senders):

                @pl.when(me != p)
                def _(p=p):
                    ex.copy(keep.at[p], kv_out.at[p], kvs.at[0], kvr.at[p], p).wait_recv()


def post_call(mesh, layer, att, hidden, gain, wo, wg, wu, wd, keep, cid):
    group = mesh.shape["sp"]
    rows, width = hidden.shape
    ff = wg.shape[2]
    tn, tf, td = 512, 512, 256
    n_o, n_f, n_d = width // tn, ff // tf, width // td
    senders = 0 if keep is None else group * 3 // 4
    whole = pl.BlockSpec((rows, width), lambda i: (0, 0), pipeline_mode=pl.Buffered(1))
    f_map = lambda i: (layer, 0, jnp.clip(i - n_o, 0, n_f - 1))
    in_specs = [
        whole,
        whole,
        pl.BlockSpec(gain.shape, lambda i: (0, 0), pipeline_mode=pl.Buffered(1)),
        pl.BlockSpec((1, width, tn), lambda i: (layer, 0, jnp.minimum(i, n_o - 1))),
        pl.BlockSpec((1, width, tf), f_map),
        pl.BlockSpec((1, width, tf), f_map),
        pl.BlockSpec((1, ff, td), lambda i: (layer, 0, jnp.clip(i - n_o - n_f, 0, n_d - 1))),
    ]
    args = [att, hidden, gain, wo, wg, wu, wd]
    out_specs = [pl.BlockSpec((rows, width), lambda i: (0, 0), pipeline_mode=pl.Buffered(1))]
    out_shape = [jax.ShapeDtypeStruct((rows, width), BF16)]
    scratch = [
        pltpu.VMEM((rows, width), BF16),
        pltpu.VMEM((rows, width), BF16),
        pltpu.VMEM((n_f, rows, tf), BF16),
    ]
    if senders:
        in_specs.append(pl.BlockSpec(memory_space=pl.ANY))
        args.append(keep)
        out_specs.append(pl.BlockSpec(memory_space=pl.ANY))
        out_shape.append(jax.ShapeDtypeStruct((senders,) + keep.shape[1:], BF16))
        scratch += [
            pltpu.SemaphoreType.DMA((group,)),
            pltpu.SemaphoreType.DMA((group,)),
            pltpu.SemaphoreType.DMA,
        ]

    def body(*refs):
        post_kernel(group, layer, (n_o, n_f, n_d), senders, refs)

    return pl.pallas_call(
        body,
        grid=(n_o + n_f + n_d,),
        in_specs=in_specs,
        out_specs=out_specs,
        out_shape=out_shape,
        scratch_shapes=scratch,
        compiler_params=params(cid if senders else None),
        name=f"post{layer}",
    )(*args)


def solution(mesh):
    row_spec = P(("dp", "sp"), None)

    def local_step(hidden, memory, mem_len, norm_self, norm_cross, norm_mlp, self_q, self_k, self_v, self_o, cross_q, cross_k, cross_v, cross_o, mlp_gate, mlp_up, mlp_down):
        layers, _, hd, width = self_o.shape
        self_o = self_o.reshape(layers, -1, width)
        cross_o = cross_o.reshape(layers, -1, width)
        keep = None
        for layer in range(layers):
            if layer == 0:
                qkv, kv, keep = qkv_call(mesh, layer, hidden, norm_self, (self_q, self_k, self_v), memory, cross_k, cross_v)
            else:
                (qkv,) = qkv_call(mesh, layer, hidden, norm_self, (self_q, self_k, self_v))
            att = self_call(mesh, hd, qkv, layers)
            hidden, q = cross_q_call(mesh, layer, att, hidden, norm_cross, self_o, cross_q, layers + 1 + layer)
            att = cross_call(mesh, hd, mem_len, q, kv.reshape(-1, 2 * hd), 2 * layers + 1)
            res = post_call(mesh, layer, att, hidden, norm_mlp, cross_o, mlp_gate, mlp_up, mlp_down, keep, 2 * layers + 2)
            hidden = res[0]
            if layer == 0:
                kv, keep = res[1], None
        return hidden

    return jax.shard_map(local_step, mesh=mesh, in_specs=(row_spec, row_spec, P("dp")) + (P(),) * 14, out_specs=row_spec, check_vma=False)
```

```python
import functools

import jax
import jax.numpy as jnp
from jax import lax
from jax.experimental import pallas as pl
from jax.experimental.pallas import tpu as pltpu
from jax.sharding import PartitionSpec as P

EPS = 1e-6
NEG_BIG = -1e30
LOG2E = 1.4426950408889634
MESH = pl.DeviceIdType.MESH
VMEM_LIMIT = 66_000_000
BF16 = jnp.bfloat16
F32 = jnp.float32


def norm_rows(hidden, gain):
    h = hidden.astype(F32)
    inv = lax.rsqrt(jnp.mean(h * h, axis=-1, keepdims=True) + EPS)
    return (h * inv * gain.astype(F32)).astype(BF16)


def dot(a, b):
    return jnp.dot(a, b, preferred_element_type=F32)


def dot_t(a, b):
    return lax.dot_general(a, b, (((1,), (1,)), ((), ())), preferred_element_type=F32)


def params(collective_id, dims=1):
    return pltpu.CompilerParams(
        collective_id=collective_id,
        has_side_effects=collective_id is not None,
        vmem_limit_bytes=VMEM_LIMIT,
        dimension_semantics=("arbitrary",) * dims,
    )


class Exchange:
    def __init__(self, group):
        self.group = group
        self.me = lax.axis_index("sp")
        self.dp = lax.axis_index("dp")

    def peer(self, offset):
        return lax.rem(self.me + offset, self.group)

    def greet(self):
        barrier = pltpu.get_barrier_semaphore()
        for k in range(1, self.group):
            pl.semaphore_signal(
                barrier, inc=1, device_id=(self.dp, self.peer(k)), device_id_type=MESH
            )

    def await_all(self):
        pl.semaphore_wait(pltpu.get_barrier_semaphore(), self.group - 1)

    def copy(self, src, dst, send, recv, target):
        return pltpu.make_async_remote_copy(
            src_ref=src, dst_ref=dst, send_sem=send, recv_sem=recv,
            device_id=(self.dp, target), device_id_type=MESH,
        )


class Stream:
    def __init__(self, ring, sems, phases):
        self.ring, self.sems, self.phases = ring, sems, phases
        self.depth = ring.shape[0]
        self.total = sum(n for n, _ in phases)

    def copies(self, phase, start, step, slot):
        return [
            pltpu.make_async_copy(src, self.ring.at[slot, pl.ds(0, src.shape[0]), cols], self.sems.at[slot, k])
            for k, (src, cols) in enumerate(self.phases[phase][1](step - start))
        ]

    def ranges(self):
        first = 0
        for phase, (n, _) in enumerate(self.phases):
            yield phase, first, first + n
            first += n

    def fetch(self, step):
        slot = lax.rem(step, self.depth)
        for phase, a, b in self.ranges():

            @pl.when((step >= a) & (step < b))
            def _(phase=phase, a=a):
                for cp in self.copies(phase, a, step, slot):
                    cp.start()

    def begin(self, i):
        @pl.when(i == 0)
        def _():
            lax.fori_loop(0, self.depth - 1, lambda k, c: (self.fetch(k), c)[1], 0)

        self.fetch(i + self.depth - 1)
        slot = lax.rem(i, self.depth)
        for phase, a, b in self.ranges():

            @pl.when((i >= a) & (i < b))
            def _(phase=phase, a=a):
                for cp in self.copies(phase, a, i, slot):
                    cp.wait()

        return slot


def cols_at(j, width):
    return pl.ds(pl.multiple_of(j * width, width), width)


def ring_scratch(depth, rows, cols, parts):
    return [pltpu.VMEM((depth, rows, cols), BF16), pltpu.SemaphoreType.DMA((depth, parts))]


def qkv_kernel(group, layer, mem_layers, refs):
    n_w = 3
    it = iter(refs)
    hid, gain = next(it), next(it)
    w = [next(it) for _ in range(n_w)]
    if mem_layers:
        mem, ck, cv = next(it), next(it), next(it)
    out = next(it)
    if mem_layers:
        kv_out, kv_keep = next(it), next(it)
    x, ring, ring_sem, buf, ssem, rsem, lsem = (next(it) for _ in range(7))
    if mem_layers:
        mem_v, kv_buf, kvs, kvr, kvl, keep_sem, mem_sem = (next(it) for _ in range(7))
    ex = Exchange(group)
    me = ex.me
    i = pl.program_id(0)
    rows = hid.shape[0]
    width = buf.shape[2]
    n_q = n_w * group
    pairs = group // 2

    phases = [(group, lambda j, t=t: [(w[t].at[layer, :, cols_at(ex.peer(j + 1), width)], slice(0, width))]) for t in range(n_w)]
    if mem_layers:
        hd2 = width // 2
        phases.append((
            mem_layers * pairs,
            lambda j: [
                (c.at[lax.div(j, pairs), :, cols_at(lax.rem(j, pairs), hd2)], slice(k * hd2, (k + 1) * hd2))
                for k, c in enumerate((ck, cv))
            ],
        ))
    stream = Stream(ring, ring_sem, phases)
    last = stream.total

    @pl.when(i == 0)
    def _():
        ex.greet()
        if mem_layers:
            pltpu.make_async_copy(mem, mem_v, mem_sem).start()

    slot = stream.begin(i)

    @pl.when(i == 0)
    def _():
        x[...] = norm_rows(hid[...], gain[layer : layer + 1, :])

    @pl.when(i == 1)
    def _():
        ex.await_all()

    def out_at(t, p):
        return out.at[t, pl.ds(pl.multiple_of(p * rows, rows), rows)]

    def own_copy(t):
        return pltpu.make_async_copy(buf.at[t * group + group - 1], out_at(t, me), lsem.at[t])

    @pl.when((i >= 1) & (i <= n_q))
    def _():
        b = i - 1
        t, r = lax.div(b, group), lax.rem(b, group)

        @pl.when(r < group - 1)
        def _():
            ex.copy(buf.at[b], out_at(t, me), ssem.at[b], rsem.at[t, me], ex.peer(r + 1)).start()

        @pl.when(r == group - 1)
        def _():
            own_copy(t).start()

    @pl.when(i < n_q)
    def _():
        buf[i] = dot(x[...], ring[slot]).astype(BF16)

    if mem_layers:
        hd = width // 4
        mem_rows = mem.shape[0]
        senders = kv_out.shape[0]

        @pl.when(i == n_q)
        def _():
            pltpu.make_async_copy(mem, mem_v, mem_sem).wait()

        def kv_copy(d):
            return ex.copy(kv_buf.at[0, d], kv_out.at[me], kvs.at[d], kvr.at[me], d)

        keep_copy = pltpu.make_async_copy(kv_buf.at[1], kv_keep, keep_sem)

        @pl.when((i > n_q) & (i <= n_q + pairs) & (me < senders))
        def _():
            for side in range(2):
                d = 2 * (i - n_q - 1) + side

                @pl.when(d != me)
                def _():
                    kv_copy(d).start()

                @pl.when(d == me)
                def _():
                    pltpu.make_async_copy(kv_buf.at[0, d], kv_out.at[me], kvl).start()

        @pl.when((i >= n_q) & (i < last) & (me < senders))
        def _():
            j = i - n_q
            m, pair = lax.div(j, pairs), lax.rem(j, pairs)
            for c in range(4):
                rs = slice(c * mem_rows // 4, (c + 1) * mem_rows // 4)
                res = dot(mem_v[rs, :], ring[slot]).astype(BF16)
                for side in range(2):
                    kv_buf[m, 2 * pair + side, rs, 0:hd] = res[:, side * hd : (side + 1) * hd]
                    kv_buf[m, 2 * pair + side, rs, hd : 2 * hd] = res[:, (2 + side) * hd : (3 + side) * hd]

        @pl.when((i == last) & (me < senders))
        def _():
            keep_copy.start()

    @pl.when(i == last)
    def _():
        for t in range(n_w):
            own_copy(t).wait()
            for k in range(1, group):
                p = ex.peer(k)
                ex.copy(buf.at[0], out_at(t, p), ssem.at[t * group + k - 1], rsem.at[t, p], p).wait()
        if mem_layers:

            @pl.when(me < senders)
            def _():
                pltpu.make_async_copy(kv_buf.at[0, 0], kv_out.at[me], kvl).wait()
                for k in range(1, group):
                    kv_copy(ex.peer(k)).wait_send()
                keep_copy.wait()

            for p in range(senders):

                @pl.when(me != p)
                def _(p=p):
                    ex.copy(kv_buf.at[0, 0], kv_out.at[p], kvs.at[0], kvr.at[p], p).wait_recv()


ANY = pl.BlockSpec(memory_space=pl.ANY)


def held(shape):
    return pl.BlockSpec(shape, lambda i: (0,) * len(shape), pipeline_mode=pl.Buffered(1))


def qkv_call(mesh, layer, hidden, gain, ws, mem=None, ck=None, cv=None):
    group = mesh.shape["sp"]
    rows, width = hidden.shape
    per_dev = ws[0].shape[2] // group
    steps = 3 * group
    mem_layers = 0 if mem is None else ck.shape[0]
    in_specs = [held((rows, width)), held(gain.shape)] + [ANY] * 3
    args = [hidden, gain, *ws]
    out_shape = [jax.ShapeDtypeStruct((3, rows * group, per_dev), BF16)]
    scratch = [pltpu.VMEM((rows, width), BF16)] + ring_scratch(4, width, per_dev, 2) + [
        pltpu.VMEM((3 * group, rows, per_dev), BF16),
        pltpu.SemaphoreType.DMA((3 * group,)),
        pltpu.SemaphoreType.DMA((3, group)),
        pltpu.SemaphoreType.DMA((3,)),
    ]
    if mem_layers:
        mem_rows = mem.shape[0]
        hd = ck.shape[2] // group
        senders = group * 3 // 4
        in_specs += [ANY] * 3
        args += [mem, ck, cv]
        out_shape += [
            jax.ShapeDtypeStruct((senders, mem_rows, 2 * hd), BF16),
            jax.ShapeDtypeStruct((group, mem_rows, 2 * hd), BF16),
        ]
        scratch += [
            pltpu.VMEM((mem_rows, width), BF16),
            pltpu.VMEM((2, group, mem_rows, 2 * hd), BF16),
            pltpu.SemaphoreType.DMA((group,)),
            pltpu.SemaphoreType.DMA((group,)),
            pltpu.SemaphoreType.DMA,
            pltpu.SemaphoreType.DMA,
            pltpu.SemaphoreType.DMA,
        ]
        steps += mem_layers * group // 2

    def body(*refs):
        qkv_kernel(group, layer, mem_layers, refs)

    return pl.pallas_call(
        body,
        grid=(steps + 1,),
        in_specs=in_specs,
        out_specs=[ANY] * len(out_shape),
        out_shape=out_shape,
        scratch_shapes=scratch,
        compiler_params=params(layer),
        name=f"qkv{layer}",
    )(*args)


def send_back(ex, i, group, rows, cols, buf, out, ssem, rsem, lsem):
    me = ex.me

    def out_at(p):
        return out.at[:, pl.ds(pl.multiple_of(p * cols, cols), cols)]

    own = pltpu.make_async_copy(buf.at[group - 1], out_at(me), lsem)

    @pl.when((i >= 1) & (i < group))
    def _():
        r = i - 1
        ex.copy(buf.at[r], out_at(me), ssem.at[r], rsem.at[me], ex.peer(r + 1)).start()

    @pl.when(i == group)
    def _():
        own.start()
        for k in range(1, group):
            p = ex.peer(k)
            ex.copy(buf.at[k - 1], out_at(p), ssem.at[k - 1], rsem.at[p], p).wait()
        own.wait()


def back_scratch(group, rows, cols):
    return [
        pltpu.VMEM((group, rows, cols), BF16),
        pltpu.SemaphoreType.DMA((group,)),
        pltpu.SemaphoreType.DMA((group,)),
        pltpu.SemaphoreType.DMA,
    ]


def soft_start(heads, rows, hd):
    return tuple(
        (jnp.full((1, rows), NEG_BIG, F32), jnp.zeros((1, rows), F32), jnp.zeros((hd, rows), F32))
        for _ in range(heads)
    )


def soft_block(carry, scores, ahead, values, coef, ss):
    heads = len(carry)
    out = []
    late = None

    def land(late):
        m, l, acc, alpha, p, h = late
        out.append((m, l, acc * alpha + dot(values(h), p)))

    for h in range(heads):
        s = ss[h % 2]
        coming = scores(h + 1) if h + 1 < heads else ahead()
        m_old, l, acc = carry[h]
        m_new = jnp.maximum(m_old, jnp.max(s, axis=0, keepdims=True))
        p = jnp.exp2((s - m_new) * coef)
        alpha = jnp.exp2((m_old - m_new) * coef)
        l_new = l * alpha + jnp.sum(p, axis=0, keepdims=True)
        p = p.astype(BF16)
        if late is not None:
            land(late)
        if coming is not None:
            ss[(h + 1) % 2] = coming
        late = (m_new, l_new, acc, alpha, p, h)
    land(late)
    return tuple(out)


def soft_finish(carry, hd, buf, i):
    for h, (_, l, acc) in enumerate(carry):
        buf[i, :, h * hd : (h + 1) * hd] = (acc / l).T.astype(BF16)


def self_kernel(group, hd, qkv, out, buf, ssem, rsem, lsem, vt, ss):
    ex = Exchange(group)
    i = pl.program_id(0)
    rows, cols = buf.shape[1], buf.shape[2]
    heads = cols // hd
    bk = 2 * rows
    coef = hd**-0.5 * LOG2E

    @pl.when(i == 0)
    def _():
        ex.greet()
        for c in range(qkv.shape[1] // bk):
            cs = slice(c * bk, (c + 1) * bk)
            vt[:, cs] = qkv[2, cs, :].astype(F32).T.astype(BF16)

    @pl.when(i == 1)
    def _():
        ex.await_all()

    @pl.when(i < group)
    def _():
        d = ex.peer(i + 1)
        r0 = pl.multiple_of(d * rows, rows)

        def heads_of(h):
            return slice(h * hd, (h + 1) * hd)

        def step(kb, carry, masked):
            k0 = pl.multiple_of(kb * bk, bk)

            def scores(h, k0=k0):
                s = dot_t(qkv[1, pl.ds(k0, bk), heads_of(h)], qkv[0, pl.ds(r0, rows), heads_of(h)])
                return jnp.where(allowed, s, NEG_BIG) if masked else s

            if masked:
                col = k0 + lax.broadcasted_iota(jnp.int32, (bk, rows), 0)
                row = r0 + lax.broadcasted_iota(jnp.int32, (bk, rows), 1)
                allowed = row >= col
            ss[0] = scores(0)
            return soft_block(carry, scores, lambda: None, lambda h: vt[heads_of(h), pl.ds(k0, bk)], coef, ss)

        full = lax.div(d, 2)
        carry = lax.fori_loop(0, full, lambda kb, c: step(kb, c, False), soft_start(heads, rows, hd))
        carry = step(full, carry, True)
        soft_finish(carry, hd, buf, i)

    send_back(ex, i, group, rows, cols, buf, out, ssem, rsem, lsem)


def self_call(mesh, hd, qkv, cid):
    group = mesh.shape["sp"]
    _, all_rows, cols = qkv.shape
    rows = all_rows // group
    return pl.pallas_call(
        functools.partial(self_kernel, group, hd),
        grid=(group + 1,),
        in_specs=[held(qkv.shape)],
        out_specs=ANY,
        out_shape=jax.ShapeDtypeStruct((rows, cols * group), BF16),
        scratch_shapes=back_scratch(group, rows, cols)
        + [pltpu.VMEM((cols, all_rows), BF16), pltpu.VMEM((2, 2 * rows, rows), F32)],
        compiler_params=params(cid),
        name="self_attn",
    )(qkv)


def cross_kernel(group, hd, bk, mem_len, q, kv, out, buf, ssem, rsem, lsem, keys, vt, qa, ss):
    ex = Exchange(group)
    i = pl.program_id(0)
    rows, cols = buf.shape[1], buf.shape[2]
    heads = cols // hd
    coef = hd**-0.5 * LOG2E
    n_kb = kv.shape[0] // bk

    @pl.when(i == 0)
    def _():
        ex.greet()
        first = lax.broadcasted_iota(jnp.int32, (bk, hd), 1) == 0
        for c in range(n_kb):
            cs = slice(c * bk, (c + 1) * bk)
            pos = c * bk + lax.broadcasted_iota(jnp.int32, (bk, hd), 0)
            keys[cs, 0:hd] = kv[cs, 0:hd]
            keys[cs, hd : 2 * hd] = jnp.where(first & (pos >= mem_len[0]), NEG_BIG, 0.0).astype(BF16)
            vt[:, cs] = kv[cs, hd : 2 * hd].astype(F32).T.astype(BF16)
        for h in range(heads):
            one = lax.broadcasted_iota(jnp.int32, (rows, hd), 1) == 0
            qa[h, :, hd : 2 * hd] = jnp.where(one, 1.0, 0.0).astype(BF16)

    @pl.when(i == 1)
    def _():
        ex.await_all()

    @pl.when(i < group)
    def _():
        r0 = pl.multiple_of(ex.peer(i + 1) * rows, rows)
        for h in range(heads):
            qa[h, :, 0:hd] = q[pl.ds(r0, rows), h * hd : (h + 1) * hd]
        ss[0] = dot_t(keys[0:bk, :], qa[0])

        def step(kb, carry):
            k0 = pl.multiple_of(kb * bk, bk)
            after = pl.multiple_of(jnp.minimum(k0 + bk, (n_kb - 1) * bk), bk)
            return soft_block(
                carry,
                lambda h: dot_t(keys[pl.ds(k0, bk), :], qa[h]),
                lambda: dot_t(keys[pl.ds(after, bk), :], qa[0]),
                lambda h: vt[:, pl.ds(k0, bk)],
                coef,
                ss,
            )

        soft_finish(lax.fori_loop(0, n_kb, step, soft_start(heads, rows, hd)), hd, buf, i)

    send_back(ex, i, group, rows, cols, buf, out, ssem, rsem, lsem)


def cross_call(mesh, hd, mem_len, q, kv, cid, used, bk):
    group = mesh.shape["sp"]
    all_rows, cols = q.shape
    rows = all_rows // group
    heads = cols // hd
    return pl.pallas_call(
        functools.partial(cross_kernel, group, hd, bk),
        grid=(group + 1,),
        in_specs=[pl.BlockSpec(memory_space=pltpu.SMEM), held(q.shape), held((used, 2 * hd))],
        out_specs=ANY,
        out_shape=jax.ShapeDtypeStruct((rows, cols * group), BF16),
        scratch_shapes=back_scratch(group, rows, cols)
        + [
            pltpu.VMEM((used, 2 * hd), BF16),
            pltpu.VMEM((hd, used), BF16),
            pltpu.VMEM((heads, rows, 2 * hd), BF16),
            pltpu.VMEM((2, bk, rows), F32),
        ],
        compiler_params=params(cid),
        name=f"cross_attn{used}",
    )(mem_len, q, kv)


LENGTHS = ((3072, 1536), (4096, 2048), (5120, 2560), (6144, 2048))


def cross_any(mesh, hd, mem_len, q, kv, cid):
    index = sum((mem_len[0] > used).astype(jnp.int32) for used, _ in LENGTHS[:-1])
    branches = [
        functools.partial(lambda used, bk, cid, m, a, b: cross_call(mesh, hd, m, a, b, cid, used, bk), used, bk, cid + n)
        for n, (used, bk) in enumerate(LENGTHS)
    ]
    return lax.switch(index, branches, mem_len, q, kv)


def cross_q_kernel(group, layer, att, hid, gain, wo, wq, out, q_out, x, ring, ring_sem, buf, ssem, rsem, lsem):
    ex = Exchange(group)
    me = ex.me
    i = pl.program_id(0)
    rows = hid.shape[0]
    tn = ring.shape[2]
    n_o = hid.shape[1] // tn

    @pl.when(i == 0)
    def _():
        ex.greet()

    stream = Stream(ring, ring_sem, [
        (n_o, lambda j: [(wo.at[layer, :, cols_at(j, tn)], slice(0, tn))]),
        (group, lambda j: [(wq.at[layer, :, cols_at(ex.peer(j + 1), tn)], slice(0, tn))]),
    ])
    slot = stream.begin(i)

    @pl.when(i < n_o)
    def _():
        cs = cols_at(i, tn)
        out[:, cs] = (hid[:, cs].astype(F32) + dot(att[...], ring[slot])).astype(BF16)

    @pl.when(i == n_o)
    def _():
        ex.await_all()
        x[...] = norm_rows(out[...], gain[layer : layer + 1, :])

    def out_at(p):
        return q_out.at[pl.ds(pl.multiple_of(p * rows, rows), rows)]

    own = pltpu.make_async_copy(buf.at[group - 1], out_at(me), lsem)

    @pl.when((i > n_o) & (i < n_o + group))
    def _():
        r = i - n_o - 1
        ex.copy(buf.at[r], out_at(me), ssem.at[r], rsem.at[me], ex.peer(r + 1)).start()

    @pl.when((i >= n_o) & (i < n_o + group))
    def _():
        buf[i - n_o] = dot(x[...], ring[slot]).astype(BF16)

    @pl.when(i == n_o + group)
    def _():
        own.start()
        for k in range(1, group):
            p = ex.peer(k)
            ex.copy(buf.at[k - 1], out_at(p), ssem.at[k - 1], rsem.at[p], p).wait()
        own.wait()


def cross_q_call(mesh, layer, att, hidden, gain, wo, wq, cid):
    group = mesh.shape["sp"]
    rows, width = hidden.shape
    tn = wq.shape[2] // group
    n_o = width // tn
    return pl.pallas_call(
        functools.partial(cross_q_kernel, group, layer),
        grid=(n_o + group + 1,),
        in_specs=[held((rows, width)), held((rows, width)), held(gain.shape), ANY, ANY],
        out_specs=[held((rows, width)), ANY],
        out_shape=[
            jax.ShapeDtypeStruct((rows, width), BF16),
            jax.ShapeDtypeStruct((rows * group, tn), BF16),
        ],
        scratch_shapes=[pltpu.VMEM((rows, width), BF16)]
        + ring_scratch(5, width, tn, 1)
        + back_scratch(group, rows, tn),
        compiler_params=params(cid),
        name=f"cross_q{layer}",
    )(att, hidden, gain, wo, wq)


def post_kernel(group, layer, senders, refs):
    it = iter(refs)
    att, hid, gain, wo, wg, wu, wd = (next(it) for _ in range(7))
    keep = next(it) if senders else None
    out = next(it)
    kv_out = next(it) if senders else None
    y, x, act, acc, ring, ring_sem = (next(it) for _ in range(6))
    i = pl.program_id(0)
    width = hid.shape[1]
    ff = act.shape[1]
    tn = ring.shape[2]
    tf = tn // 2
    parts = 4
    tk = ff // parts
    n_o, n_f, n_d = width // tn, ff // tf, width // tn * parts
    last = n_o + n_f + n_d - 1
    if senders:
        kvs, kvr, kvl = (next(it) for _ in range(3))
        ex = Exchange(group)
        me = ex.me

        def kv_copy(d):
            return ex.copy(keep.at[d], kv_out.at[me], kvs.at[d], kvr.at[me], d)

        own = pltpu.make_async_copy(keep.at[me], kv_out.at[me], kvl)

        @pl.when(i == 0)
        def _():
            ex.greet()

    stream = Stream(ring, ring_sem, [
        (n_o, lambda j: [(wo.at[layer, :, cols_at(j, tn)], slice(0, tn))]),
        (n_f, lambda j: [
            (wg.at[layer, :, cols_at(j, tf)], slice(0, tf)),
            (wu.at[layer, :, cols_at(j, tf)], slice(tf, tn)),
        ]),
        (n_d, lambda j: [(
            wd.at[layer, pl.ds(pl.multiple_of(lax.rem(j, parts) * tk, tk), tk), cols_at(lax.div(j, parts), tn)],
            slice(0, tn),
        )]),
    ])
    slot = stream.begin(i)

    if senders:

        @pl.when(i == 1)
        def _():
            ex.await_all()

        @pl.when((i == 1) & (me < senders))
        def _():
            own.start()
            for k in range(1, group):
                kv_copy(ex.peer(k)).start()

    @pl.when(i < n_o)
    def _():
        cs = cols_at(i, tn)
        y[:, cs] = (hid[:, cs].astype(F32) + dot(att[...], ring[slot])).astype(BF16)

    @pl.when(i == n_o)
    def _():
        x[...] = norm_rows(y[...], gain[layer : layer + 1, :])

    @pl.when((i >= n_o) & (i < n_o + n_f))
    def _():
        g = dot(x[...], ring[slot, :, 0:tf])
        u = dot(x[...], ring[slot, :, tf:tn])
        act[:, cols_at(i - n_o, tf)] = (g * jax.nn.sigmoid(g) * u).astype(BF16)

    @pl.when(i >= n_o + n_f)
    def _():
        j = i - n_o - n_f
        part, block = lax.rem(j, parts), lax.div(j, parts)
        prod = dot(act[:, pl.ds(pl.multiple_of(part * tk, tf), tk)], ring[slot, 0:tk, :])

        @pl.when(part == 0)
        def _():
            acc[...] = prod

        @pl.when(part > 0)
        def _():
            acc[...] += prod

        @pl.when(part == parts - 1)
        def _():
            cs = cols_at(block, tn)
            out[:, cs] = (y[:, cs].astype(F32) + acc[...]).astype(BF16)

    if senders:

        @pl.when(i == last)
        def _():
            @pl.when(me < senders)
            def _():
                own.wait()
                for k in range(1, group):
                    kv_copy(ex.peer(k)).wait_send()

            for p in range(senders):

                @pl.when(me != p)
                def _(p=p):
                    ex.copy(keep.at[p], kv_out.at[p], kvs.at[0], kvr.at[p], p).wait_recv()


def post_call(mesh, layer, att, hidden, gain, wo, wg, wu, wd, keep, cid):
    group = mesh.shape["sp"]
    rows, width = hidden.shape
    ff = wg.shape[2]
    tn = 1024
    senders = 0 if keep is None else group * 3 // 4
    in_specs = [held((rows, width)), held((rows, width)), held(gain.shape)] + [ANY] * 4
    args = [att, hidden, gain, wo, wg, wu, wd]
    out_specs = [held((rows, width))]
    out_shape = [jax.ShapeDtypeStruct((rows, width), BF16)]
    scratch = [
        pltpu.VMEM((rows, width), BF16),
        pltpu.VMEM((rows, width), BF16),
        pltpu.VMEM((rows, ff), BF16),
        pltpu.VMEM((rows, tn), F32),
    ] + ring_scratch(3, width, tn, 2)
    if senders:
        in_specs.append(ANY)
        args.append(keep)
        out_specs.append(ANY)
        out_shape.append(jax.ShapeDtypeStruct((senders,) + keep.shape[1:], BF16))
        scratch += [
            pltpu.SemaphoreType.DMA((group,)),
            pltpu.SemaphoreType.DMA((group,)),
            pltpu.SemaphoreType.DMA,
        ]

    def body(*refs):
        post_kernel(group, layer, senders, refs)

    return pl.pallas_call(
        body,
        grid=(width // tn + ff // (tn // 2) + width // tn * 4,),
        in_specs=in_specs,
        out_specs=out_specs,
        out_shape=out_shape,
        scratch_shapes=scratch,
        compiler_params=params(cid if senders else None),
        name=f"post{layer}",
    )(*args)


def solution(mesh):
    row_spec = P(("dp", "sp"), None)

    def local_step(hidden, memory, mem_len, norm_self, norm_cross, norm_mlp, self_q, self_k, self_v, self_o, cross_q, cross_k, cross_v, cross_o, mlp_gate, mlp_up, mlp_down):
        layers, _, hd, width = self_o.shape
        self_o = self_o.reshape(layers, -1, width)
        cross_o = cross_o.reshape(layers, -1, width)
        keep = None
        for layer in range(layers):
            if layer == 0:
                qkv, kv, keep = qkv_call(mesh, layer, hidden, norm_self, (self_q, self_k, self_v), memory, cross_k, cross_v)
            else:
                (qkv,) = qkv_call(mesh, layer, hidden, norm_self, (self_q, self_k, self_v))
            att = self_call(mesh, hd, qkv, layers)
            hidden, q = cross_q_call(mesh, layer, att, hidden, norm_cross, self_o, cross_q, layers + 1 + layer)
            att = cross_any(mesh, hd, mem_len, q, kv.reshape(-1, 2 * hd), 2 * layers + 2)
            res = post_call(mesh, layer, att, hidden, norm_mlp, cross_o, mlp_gate, mlp_up, mlp_down, keep, 2 * layers + 1)
            hidden = res[0]
            if layer == 0:
                kv, keep = res[1], None
        return hidden

    return jax.shard_map(local_step, mesh=mesh, in_specs=(row_spec, row_spec, P("dp")) + (P(),) * 14, out_specs=row_spec, check_vma=False)
```
